32 devices in a mesh: row: 4 (over y, x), col: 8 (over z, core).
Axes of the slice: x: 2, y: 2, z: 4, core: 2. Of those that a mesh axis runs over, the one named last changes fastest.
Arguments:
- matrix: float32 [2, 4, 256, 1, 8, 256], P(None, 'row', None, None, 'col'), as said below
Outputs:
- factored: float32 [2, 4, 256, 1, 8, 256], P(None, 'row', None, None, 'col')
Inputs may be any that keep to these rules, and one draw needn't show every extreme that they name: `matrix`: symmetric and positive definite.
All inputs are finite; a program needn't handle non-finite values.
Results may differ from the reference program's by a relative error of at most 0.0001.
Values sent between devices are 32-bit elements; how exact they have to be, the bound alone decides.
A program may use at most 128 MiB of HBM per device.

```python
import jax
import jax.numpy as jnp
from jax import lax

B = 256
MR = 2
STEPS = 8
MC = 1
N_ROW = 4
N_COL = 8


def draw_matrix(key, part):
    order = MR * N_ROW * B
    inner_count = order // 4
    first, second = jax.random.split(key, 2)
    factor_g = jax.random.normal(first, (order, inner_count), jnp.float32)
    product = jnp.dot(factor_g, factor_g.T, precision=lax.Precision.HIGHEST, preferred_element_type=jnp.float32)
    product = product * (1.0 / inner_count)
    product = 0.5 * (product + product.T)
    diag_vals = jax.random.uniform(second, (order,), jnp.float32, 0.5, 1.5)
    result = product + jnp.diag(diag_vals)
    return result.reshape(MR, N_ROW, B, MC, N_COL, B)


def setup_inputs(seed: int = 0) -> dict:
    streams_of = jax.random.split(jax.random.key(seed), 2)
    return {
        "matrix": draw_matrix(jax.random.fold_in(streams_of[1], 71), 0),
    }


def reference(matrix):
    order = MR * N_ROW * B
    work = matrix.reshape(order, order)
    for k in range(STEPS):
        low = k * B
        high = low + B
        factor = jnp.linalg.cholesky(work[low:high, low:high])
        below = work[high:, low:high]
        solved = jax.scipy.linalg.solve_triangular(factor, below.T, lower=True).T
        update = jnp.dot(solved.astype(jnp.float32), solved.T.astype(jnp.float32), precision=lax.Precision.HIGHEST, preferred_element_type=jnp.float32)
        work = work.at[high:, high:].add(-update)
        work = work.at[:low, low:high].set(jnp.zeros((low, B), jnp.float32))
        work = work.at[low:high, low:high].set(factor)
        work = work.at[high:, low:high].set(solved)
    return work.reshape(matrix.shape)
```

```python
import functools

import jax
import jax.numpy as jnp
from jax import lax
from jax.experimental import pallas as pl
from jax.experimental.pallas import tpu as pltpu
from jax.sharding import PartitionSpec as P

STEPS = 8
LANES = 128
SUBS = 8
PANEL = 32
MESH = pl.DeviceIdType.MESH
NT = (((1,), (1,)), ((), ()))
TN = (((0,), (0,)), ((), ()))


def split(value):
    high = value.astype(jnp.bfloat16)
    low = (value - high.astype(jnp.float32)).astype(jnp.bfloat16)
    return high, low


def dot3(a_high, a_low, b_high, b_low):
    def one(a, b):
        return lax.dot_general(a, b, NT, preferred_element_type=jnp.float32)

    return one(a_high, b_high) + (one(a_high, b_low) + one(a_low, b_high))


def factor_panel(work, width, base, start):
    groups = PANEL // SUBS
    chunks = (width + LANES) // LANES
    offset = start - base
    shape = (SUBS, LANES)
    sub = lax.broadcasted_iota(jnp.int32, shape, 0)
    rows = []
    for g in range(groups):
        at = pl.ds(pl.multiple_of(start + g * SUBS, SUBS), SUBS)
        row = [work[at, base + h * LANES : base + (h + 1) * LANES] for h in range(chunks)]
        row.append(pltpu.roll(row[0], lax.rem(LANES - offset, LANES), 1))
        rows.append(row)
    for b in range(groups):
        lane = b * SUBS
        cols = [
            [jnp.broadcast_to(rows[g][chunks][:, lane + t : lane + t + 1], shape) for g in range(b, groups)]
            for t in range(SUBS)
        ]
        scales = jnp.ones(shape, jnp.float32)
        for t in range(SUBS):
            scale = lax.rsqrt(jnp.broadcast_to(cols[t][0][t : t + 1, :], shape))
            scales = jnp.where(sub == t, scale, scales)
            mult = [c * scale for c in cols[t]]
            for r in range(t + 1, SUBS):
                across = jnp.broadcast_to(mult[0][r : r + 1, :], shape)
                cols[r] = [c - m * across for c, m in zip(cols[r], mult)]
            below = jnp.where(sub > t, mult[0], 0.0)
            for h in range(chunks + 1):
                pivot = jnp.broadcast_to(rows[b][h][t : t + 1, :], shape) * scale
                rows[b][h] = rows[b][h] - below * pivot
                for g in range(b + 1, groups):
                    rows[g][h] = rows[g][h] - mult[g - b] * pivot
        rows[b] = [r * scales for r in rows[b]]
    for g in range(groups):
        at = pl.ds(pl.multiple_of(start + g * SUBS, SUBS), SUBS)
        for h in range(chunks):
            work[at, base + h * LANES : base + (h + 1) * LANES] = rows[g][h]
    whole = jnp.concatenate([jnp.concatenate(row[:chunks], 1) for row in rows], 0)
    high, low = split(whole)
    rest = width - base
    left = whole[:, :rest]
    left = jnp.where(lax.broadcasted_iota(jnp.int32, left.shape, 1) >= offset + PANEL, left, 0.0)
    left_high, left_low = split(left)
    update = lax.dot_general(
        jnp.concatenate([left_high, left_high, left_low], 0),
        jnp.concatenate([high, low, high], 0),
        TN,
        preferred_element_type=jnp.float32,
    )
    work[base:width, base : base + width + LANES] -= update


def factor_tile(work, width):
    for base in range(0, width, LANES):
        def one(i, carry, base=base):
            factor_panel(work, width, base, base + i * PANEL)
            return carry

        lax.fori_loop(0, LANES // PANEL, one, 0)


def kernel(dims, x_ref, o_ref, tiles, high, low, work, inv_high, inv_low, in_sem, out_sem, send_sem, land_sem):
    steps, num_row, num_col = dims
    row_tiles, width, _ = x_ref.shape
    my_row, my_col = lax.axis_index("row"), lax.axis_index("col")
    root = jnp.logical_and(my_row == 0, my_col == 0)
    count = num_row * num_col
    barrier = pltpu.get_barrier_semaphore()

    def inbound(a, i, slot, device):
        return pltpu.make_async_remote_copy(
            src_ref=x_ref.at[a], dst_ref=tiles.at[slot], send_sem=send_sem.at[a], recv_sem=in_sem.at[slot],
            device_id=device, device_id_type=MESH,
        )

    def outbound(slot, a, device):
        return pltpu.make_async_remote_copy(
            src_ref=tiles.at[slot], dst_ref=o_ref.at[a], send_sem=out_sem.at[slot], recv_sem=land_sem.at[a],
            device_id=device, device_id_type=MESH,
        )

    @pl.when(jnp.logical_not(root))
    def _():
        pl.semaphore_signal(barrier, inc=1, device_id=(0, 0), device_id_type=MESH)
        pl.semaphore_wait(barrier, 1)
        for a in range(row_tiles):
            i = a * num_row + my_row

            @pl.when(i >= my_col)
            def _():
                inbound(a, i, i * steps + my_col, (0, 0)).start()

            @pl.when(i < my_col)
            def _():
                o_ref[a] = jnp.zeros((width, width), jnp.float32)

        for a in range(row_tiles):
            i = a * num_row + my_row

            @pl.when(i >= my_col)
            def _():
                inbound(a, i, i * steps + my_col, (0, 0)).wait_send()
                outbound(0, a, (0, 0)).wait_recv()

    @pl.when(root)
    def _():
        for a in range(row_tiles):
            pltpu.make_async_copy(x_ref.at[a], tiles.at[a * num_row * steps], in_sem.at[a * num_row * steps]).start()

        def greet(d, carry):
            pl.semaphore_signal(
                barrier, inc=1, device_id=(d // num_col, lax.rem(d, num_col)), device_id_type=MESH
            )
            return carry

        lax.fori_loop(1, count, greet, 0)
        pl.semaphore_wait(barrier, count - 1)

        def arrive(slot):
            pltpu.make_async_copy(tiles.at[slot], tiles.at[slot], in_sem.at[slot]).wait()

        def owned(i, k):
            return jnp.logical_and(lax.rem(i, num_row) == 0, k == 0)

        def send(i, k):
            slot = i * steps + k

            @pl.when(owned(i, k))
            def _():
                pltpu.make_async_copy(tiles.at[slot], o_ref.at[i // num_row], out_sem.at[slot]).start()

            @pl.when(jnp.logical_not(owned(i, k)))
            def _():
                outbound(slot, i // num_row, (lax.rem(i, num_row), k)).start()

        def block(i):
            return pl.ds(pl.multiple_of(i * width, width), width)

        def subtract(i, k):
            slot = i * steps + k
            arrive(slot)

            def one(m, carry):
                tiles[slot] -= dot3(
                    high[block(i), block(m)], low[block(i), block(m)],
                    high[block(k), block(m)], low[block(k), block(m)],
                )
                return carry

            lax.fori_loop(0, k, one, 0)

        def step(k, carry):
            slot = k * steps + k
            subtract(k, k)
            rows = lax.broadcasted_iota(jnp.int32, (width, width), 0)
            cols = lax.broadcasted_iota(jnp.int32, (width, width), 1)
            work[:, :width] = tiles[slot]
            work[:, width:] = jnp.where(rows == cols, 1.0, 0.0)
            factor_tile(work, width)
            tiles[slot] = jnp.where(cols >= rows, work[:, :width], 0.0).T
            inv_high[...], inv_low[...] = split(work[:, width:])

            def panel(i, carry):
                subtract(i, k)
                spot = i * steps + k
                a_high, a_low = split(tiles[spot])
                solved = dot3(a_high, a_low, inv_high[...], inv_low[...])
                tiles[spot] = solved
                high[block(i), block(k)], low[block(i), block(k)] = split(solved)
                return carry

            lax.fori_loop(k + 1, steps, panel, 0)

            def ship(i, carry):
                send(i, k)
                return carry

            lax.fori_loop(k, steps, ship, 0)
            return carry

        lax.fori_loop(0, steps, step, 0)

        def finish(k, carry):
            def one(i, carry):
                slot = i * steps + k
                pltpu.make_async_copy(tiles.at[slot], tiles.at[slot], out_sem.at[slot]).wait()
                return carry

            return lax.fori_loop(k, steps, one, carry)

        lax.fori_loop(0, steps, finish, 0)


def on_root(matrix):
    row_tiles = matrix.shape[0]
    width = matrix.shape[2]
    num_row, num_col = lax.axis_size("row"), lax.axis_size("col")
    order = STEPS * width
    local = matrix.reshape(row_tiles, width, width)
    slots = STEPS * STEPS
    out = pl.pallas_call(
        functools.partial(kernel, (STEPS, num_row, num_col)),
        out_shape=jax.ShapeDtypeStruct(local.shape, jnp.float32),
        in_specs=[pl.BlockSpec(memory_space=pltpu.VMEM)],
        out_specs=pl.BlockSpec(memory_space=pltpu.VMEM),
        scratch_shapes=[
            pltpu.VMEM((slots, width, width), jnp.float32),
            pltpu.VMEM((order, order), jnp.bfloat16),
            pltpu.VMEM((order, order), jnp.bfloat16),
            pltpu.VMEM((width, 2 * width), jnp.float32),
            pltpu.VMEM((width, width), jnp.bfloat16),
            pltpu.VMEM((width, width), jnp.bfloat16),
            pltpu.SemaphoreType.DMA((slots,)),
            pltpu.SemaphoreType.DMA((slots,)),
            pltpu.SemaphoreType.DMA((row_tiles,)),
            pltpu.SemaphoreType.DMA((row_tiles,)),
        ],
        compiler_params=pltpu.CompilerParams(collective_id=0, has_side_effects=True, vmem_limit_bytes=56 * 2**20),
    )(local)
    return out.reshape(matrix.shape)


def broadcast(value, axis, source):
    kept = jnp.where(lax.axis_index(axis) == source, value, 0).astype(value.dtype)
    return lax.psum(kept, axis)


def solve_panel(factor, column):
    width = column.shape[1]
    inverse = jax.scipy.linalg.solve_triangular(
        factor, jnp.eye(width, dtype=jnp.float32), lower=True
    )
    solved = jnp.einsum("ts,ars->art", inverse, column, precision=lax.Precision.HIGHEST)
    return solved


def stepwise(matrix):
    row_tiles = matrix.shape[0]
    width = matrix.shape[2]
    col_tiles = matrix.shape[3]
    tile_grid = matrix.reshape(row_tiles, width, col_tiles, width)
    num_row = lax.axis_size("row")
    num_col = lax.axis_size("col")
    my_row = lax.axis_index("row")
    my_col = lax.axis_index("col")
    rows_global = jnp.arange(row_tiles, dtype=jnp.int32) * num_row + my_row
    ratio = num_col // num_row
    for k in range(STEPS):
        lead_row = k % num_row
        lead_col = k % num_col
        local_row = k // num_row
        local_col = k // num_col
        column = tile_grid[:, :, local_col, :]
        candidate = tile_grid[local_row, :, local_col, :]
        keep = (rows_global > k)[:, None, None]
        diag_tile = broadcast(candidate, "row", lead_row)
        factor = jnp.linalg.cholesky(diag_tile)
        local_panel = jnp.where(keep, solve_panel(factor, column), 0.0)
        panel_rows = broadcast(local_panel, "col", lead_col)
        grouped = panel_rows.reshape(col_tiles, ratio, width, width)
        chosen = lax.dynamic_index_in_dim(grouped, my_col // num_row, 1, keepdims=False)
        panel_cols = broadcast(chosen, "row", my_col % num_row)
        update = jnp.einsum(
            "art,bst->arbs", panel_rows, panel_cols, precision=lax.Precision.HIGHEST
        )
        tile_grid = tile_grid - update
        diagonal_part = jnp.where((rows_global == k)[:, None, None], factor[None], 0.0)
        new_column = panel_rows + diagonal_part
        old_column = tile_grid[:, :, local_col, :]
        tile_grid = tile_grid.at[:, :, local_col, :].set(
            jnp.where(my_col == lead_col, new_column, old_column)
        )
    return tile_grid.reshape(matrix.shape)


def on_device(matrix):
    row_tiles, _, _, col_tiles = matrix.shape[:4]
    whole = row_tiles * lax.axis_size("row") == STEPS and lax.axis_size("col") == STEPS and col_tiles == 1
    return on_root(matrix) if whole else stepwise(matrix)


def solution(mesh):
    placed = (P(None, "row", None, None, "col", None),)
    return jax.shard_map(
        on_device,
        mesh=mesh,
        in_specs=placed,
        out_specs=P(None, "row", None, None, "col", None),
        check_vma=False,
    )
```

```python
import functools

import jax
import jax.numpy as jnp
from jax import lax
from jax.experimental import pallas as pl
from jax.experimental.pallas import tpu as pltpu
from jax.sharding import PartitionSpec as P

STEPS = 8
LANES = 128
SUBS = 8
PANEL = 64
ROOT_COL = 2
MESH = pl.DeviceIdType.MESH
NT = (((1,), (1,)), ((), ()))
TN = (((0,), (0,)), ((), ()))


def split(value):
    high = value.astype(jnp.bfloat16)
    low = (value - high.astype(jnp.float32)).astype(jnp.bfloat16)
    return high, low


def dot3(a_high, a_low, b_high, b_low):
    def one(a, b):
        return lax.dot_general(a, b, NT, preferred_element_type=jnp.float32)

    return one(a_high, b_high) + (one(a_high, b_low) + one(a_low, b_high))


def factor_panel(work, width, base, start):
    groups = PANEL // SUBS
    chunks = (width + LANES) // LANES
    offset = start - base
    shape = (SUBS, LANES)
    sub = lax.broadcasted_iota(jnp.int32, shape, 0)
    rows = []
    for g in range(groups):
        at = pl.ds(pl.multiple_of(start + g * SUBS, SUBS), SUBS)
        row = [work[at, base + h * LANES : base + (h + 1) * LANES] for h in range(chunks)]
        row.append(pltpu.roll(row[0], lax.rem(LANES - offset, LANES), 1))
        rows.append(row)
    for b in range(groups):
        lane = b * SUBS
        cols = [
            [jnp.broadcast_to(rows[g][chunks][:, lane + t : lane + t + 1], shape) for g in range(b, groups)]
            for t in range(SUBS)
        ]
        scales = jnp.ones(shape, jnp.float32)
        for t in range(SUBS):
            scale = lax.rsqrt(jnp.broadcast_to(cols[t][0][t : t + 1, :], shape))
            scales = jnp.where(sub == t, scale, scales)
            mult = [c * scale for c in cols[t]]
            for r in range(t + 1, SUBS):
                across = jnp.broadcast_to(mult[0][r : r + 1, :], shape)
                cols[r] = [c - m * across for c, m in zip(cols[r], mult)]
            below = jnp.where(sub > t, mult[0], 0.0)
            for h in range(chunks + 1):
                pivot = jnp.broadcast_to(rows[b][h][t : t + 1, :], shape) * scale
                rows[b][h] = rows[b][h] - below * pivot
                for g in range(b + 1, groups):
                    rows[g][h] = rows[g][h] - mult[g - b] * pivot
        rows[b] = [r * scales for r in rows[b]]
    for g in range(groups):
        at = pl.ds(pl.multiple_of(start + g * SUBS, SUBS), SUBS)
        for h in range(chunks):
            work[at, base + h * LANES : base + (h + 1) * LANES] = rows[g][h]
    whole = jnp.concatenate([jnp.concatenate(row[:chunks], 1) for row in rows], 0)
    high, low = split(whole)
    rest = width - base
    left = whole[:, :rest]
    left = jnp.where(lax.broadcasted_iota(jnp.int32, left.shape, 1) >= offset + PANEL, left, 0.0)
    left_high, left_low = split(left)
    update = lax.dot_general(
        jnp.concatenate([left_high, left_high, left_low], 0),
        jnp.concatenate([high, low, high], 0),
        TN,
        preferred_element_type=jnp.float32,
    )
    work[base:width, base : base + width + LANES] -= update


def factor_tile(work, width):
    for base in range(0, width, LANES):
        def one(i, carry, base=base):
            factor_panel(work, width, base, base + i * PANEL)
            return carry

        lax.fori_loop(0, LANES // PANEL, one, 0)


def kernel(dims, x_ref, o_ref, tiles, high, low, work, inv_high, inv_low, in_sem, out_sem, send_sem, land_sem, go_sem):
    steps, num_row, num_col = dims
    row_tiles, width, _ = x_ref.shape
    my_row, my_col = lax.axis_index("row"), lax.axis_index("col")
    root_row, root_col = num_row - 1, min(ROOT_COL, num_col - 1)
    home = (root_row, root_col)
    root = jnp.logical_and(my_row == root_row, my_col == root_col)
    count = num_row * num_col
    barrier = pltpu.get_barrier_semaphore()

    def inbound(a, i, slot, device):
        return pltpu.make_async_remote_copy(
            src_ref=x_ref.at[a], dst_ref=tiles.at[slot], send_sem=send_sem.at[a], recv_sem=in_sem.at[slot],
            device_id=device, device_id_type=MESH,
        )

    def outbound(slot, a, device):
        return pltpu.make_async_remote_copy(
            src_ref=tiles.at[slot], dst_ref=o_ref.at[a], send_sem=out_sem.at[slot], recv_sem=land_sem.at[a],
            device_id=device, device_id_type=MESH,
        )

    beside = my_row == root_row
    ahead = jnp.where(jnp.logical_and(beside, my_col - 1 == root_col), my_col - 2, my_col - 1)
    after = jnp.where(jnp.logical_and(beside, my_col + 1 == root_col), my_col + 2, my_col + 1)
    follows, leads = ahead >= 0, after < num_col

    @pl.when(jnp.logical_not(root))
    def _():
        pl.semaphore_signal(barrier, inc=1, device_id=home, device_id_type=MESH)

        @pl.when(follows)
        def _():
            pl.semaphore_signal(barrier, inc=1, device_id=(my_row, ahead), device_id_type=MESH)

        pl.semaphore_wait(barrier, jnp.where(leads, 2, 1))

        @pl.when(follows)
        def _():
            pl.semaphore_wait(go_sem, 1)

        for a in range(row_tiles):
            i = a * num_row + my_row

            @pl.when(i >= my_col)
            def _():
                inbound(a, i, i * steps + my_col, home).start()

            @pl.when(i < my_col)
            def _():
                o_ref[a] = jnp.zeros((width, width), jnp.float32)

        for a in range(row_tiles):
            i = a * num_row + my_row

            @pl.when(i >= my_col)
            def _():
                inbound(a, i, i * steps + my_col, home).wait_send()

        @pl.when(leads)
        def _():
            pl.semaphore_signal(go_sem, inc=1, device_id=(my_row, after), device_id_type=MESH)

        for a in range(row_tiles):
            i = a * num_row + my_row

            @pl.when(i >= my_col)
            def _():
                outbound(0, a, home).wait_recv()

    @pl.when(root)
    def _():
        for a in range(row_tiles):
            i = a * num_row + root_row
            if i >= root_col:
                slot = i * steps + root_col
                pltpu.make_async_copy(x_ref.at[a], tiles.at[slot], in_sem.at[slot]).start()
            else:
                o_ref[a] = jnp.zeros((width, width), jnp.float32)

        def greet(d, carry):
            d = jnp.where(d >= root_row * num_col + root_col, d + 1, d)
            pl.semaphore_signal(
                barrier, inc=1, device_id=(d // num_col, lax.rem(d, num_col)), device_id_type=MESH
            )
            return carry

        lax.fori_loop(0, count - 1, greet, 0)
        pl.semaphore_wait(barrier, count - 1)

        def arrive(slot):
            pltpu.make_async_copy(tiles.at[slot], tiles.at[slot], in_sem.at[slot]).wait()

        def owned(i, k):
            return jnp.logical_and(lax.rem(i, num_row) == root_row, k == root_col)

        def send(i, k):
            slot = i * steps + k

            @pl.when(owned(i, k))
            def _():
                pltpu.make_async_copy(tiles.at[slot], o_ref.at[i // num_row], out_sem.at[slot]).start()

            @pl.when(jnp.logical_not(owned(i, k)))
            def _():
                outbound(slot, i // num_row, (lax.rem(i, num_row), k)).start()

        def block(i):
            return pl.ds(pl.multiple_of(i * width, width), width)

        def subtract(i, k):
            slot = i * steps + k
            arrive(slot)

            def one(m, carry):
                tiles[slot] -= dot3(
                    high[block(i), block(m)], low[block(i), block(m)],
                    high[block(k), block(m)], low[block(k), block(m)],
                )
                return carry

            lax.fori_loop(0, k, one, 0)

        def step(k, carry):
            slot = k * steps + k
            subtract(k, k)
            rows = lax.broadcasted_iota(jnp.int32, (width, width), 0)
            cols = lax.broadcasted_iota(jnp.int32, (width, width), 1)
            work[:, :width] = tiles[slot]
            work[:, width:] = jnp.where(rows == cols, 1.0, 0.0)
            factor_tile(work, width)
            tiles[slot] = jnp.where(cols >= rows, work[:, :width], 0.0).T
            inv_high[...], inv_low[...] = split(work[:, width:])

            def panel(i, carry):
                send(i - 1, k)
                subtract(i, k)
                spot = i * steps + k
                a_high, a_low = split(tiles[spot])
                solved = dot3(a_high, a_low, inv_high[...], inv_low[...])
                tiles[spot] = solved
                high[block(i), block(k)], low[block(i), block(k)] = split(solved)
                return carry

            lax.fori_loop(k + 1, steps, panel, 0)

            send(steps - 1, k)
            return carry

        lax.fori_loop(0, steps, step, 0)

        def finish(k, carry):
            def one(i, carry):
                slot = i * steps + k
                pltpu.make_async_copy(tiles.at[slot], tiles.at[slot], out_sem.at[slot]).wait()
                return carry

            return lax.fori_loop(k, steps, one, carry)

        lax.fori_loop(0, steps, finish, 0)


def on_root(matrix):
    row_tiles = matrix.shape[0]
    width = matrix.shape[2]
    num_row, num_col = lax.axis_size("row"), lax.axis_size("col")
    order = STEPS * width
    local = matrix.reshape(row_tiles, width, width)
    slots = STEPS * STEPS
    out = pl.pallas_call(
        functools.partial(kernel, (STEPS, num_row, num_col)),
        out_shape=jax.ShapeDtypeStruct(local.shape, jnp.float32),
        in_specs=[pl.BlockSpec(memory_space=pltpu.VMEM)],
        out_specs=pl.BlockSpec(memory_space=pltpu.VMEM),
        scratch_shapes=[
            pltpu.VMEM((slots, width, width), jnp.float32),
            pltpu.VMEM((order, order), jnp.bfloat16),
            pltpu.VMEM((order, order), jnp.bfloat16),
            pltpu.VMEM((width, 2 * width), jnp.float32),
            pltpu.VMEM((width, width), jnp.bfloat16),
            pltpu.VMEM((width, width), jnp.bfloat16),
            pltpu.SemaphoreType.DMA((slots,)),
            pltpu.SemaphoreType.DMA((slots,)),
            pltpu.SemaphoreType.DMA((row_tiles,)),
            pltpu.SemaphoreType.DMA((row_tiles,)),
            pltpu.SemaphoreType.REGULAR,
        ],
        compiler_params=pltpu.CompilerParams(collective_id=0, has_side_effects=True, vmem_limit_bytes=56 * 2**20),
    )(local)
    return out.reshape(matrix.shape)


def broadcast(value, axis, source):
    kept = jnp.where(lax.axis_index(axis) == source, value, 0).astype(value.dtype)
    return lax.psum(kept, axis)


def solve_panel(factor, column):
    width = column.shape[1]
    inverse = jax.scipy.linalg.solve_triangular(
        factor, jnp.eye(width, dtype=jnp.float32), lower=True
    )
    solved = jnp.einsum("ts,ars->art", inverse, column, precision=lax.Precision.HIGHEST)
    return solved


def stepwise(matrix):
    row_tiles = matrix.shape[0]
    width = matrix.shape[2]
    col_tiles = matrix.shape[3]
    tile_grid = matrix.reshape(row_tiles, width, col_tiles, width)
    num_row = lax.axis_size("row")
    num_col = lax.axis_size("col")
    my_row = lax.axis_index("row")
    my_col = lax.axis_index("col")
    rows_global = jnp.arange(row_tiles, dtype=jnp.int32) * num_row + my_row
    ratio = num_col // num_row
    for k in range(STEPS):
        lead_row = k % num_row
        lead_col = k % num_col
        local_row = k // num_row
        local_col = k // num_col
        column = tile_grid[:, :, local_col, :]
        candidate = tile_grid[local_row, :, local_col, :]
        keep = (rows_global > k)[:, None, None]
        diag_tile = broadcast(candidate, "row", lead_row)
        factor = jnp.linalg.cholesky(diag_tile)
        local_panel = jnp.where(keep, solve_panel(factor, column), 0.0)
        panel_rows = broadcast(local_panel, "col", lead_col)
        grouped = panel_rows.reshape(col_tiles, ratio, width, width)
        chosen = lax.dynamic_index_in_dim(grouped, my_col // num_row, 1, keepdims=False)
        panel_cols = broadcast(chosen, "row", my_col % num_row)
        update = jnp.einsum(
            "art,bst->arbs", panel_rows, panel_cols, precision=lax.Precision.HIGHEST
        )
        tile_grid = tile_grid - update
        diagonal_part = jnp.where((rows_global == k)[:, None, None], factor[None], 0.0)
        new_column = panel_rows + diagonal_part
        old_column = tile_grid[:, :, local_col, :]
        tile_grid = tile_grid.at[:, :, local_col, :].set(
            jnp.where(my_col == lead_col, new_column, old_column)
        )
    return tile_grid.reshape(matrix.shape)


def on_device(matrix):
    row_tiles, _, _, col_tiles = matrix.shape[:4]
    whole = row_tiles * lax.axis_size("row") == STEPS and lax.axis_size("col") == STEPS and col_tiles == 1
    return on_root(matrix) if whole else stepwise(matrix)


def solution(mesh):
    placed = (P(None, "row", None, None, "col", None),)
    return jax.shard_map(
        on_device,
        mesh=mesh,
        in_specs=placed,
        out_specs=P(None, "row", None, None, "col", None),
        check_vma=False,
    )
```
